32 devices in a mesh: blk: 8 (over y, x, core), grp: 4 (over z).
Axes of the slice: x: 2, y: 2, z: 4, core: 2. Of those that a mesh axis runs over, the one named last changes fastest.
Arguments:
- queries: bfloat16 [48, 8192], P(None, ('blk', 'grp')), may hold values from -6 to 6
- key_pool: bfloat16 [4, 64, 128, 1024], P('grp', 'blk'), may hold values from -28 to 28
- value_pool: bfloat16 [4, 64, 128, 1024], P('grp', 'blk'), may hold values from -6 to 6
- lengths: int32 [4, 4], P('grp'), may hold values from 1 to 32, as said below
- block_table: int32 [4, 4, 32], P('grp'), may hold values from 0 to 63, as said below
Outputs:
- attended: bfloat16 [48, 8192], P('grp', 'blk')
The draws below stay inside these ranges and needn't reach their ends.
Inputs may be any that keep to these rules, and one draw needn't show every extreme that they name: Each group's 4 lengths add up to 52, and one of them is exactly 32. Within a group, the entries block_table[g, q, j] with j < lengths[g, q] are distinct slots; entries past a sequence's length are arbitrary slots and unused. Slots s * 8 to s * 8 + 7 form the s-th aligned block of the pool; at least 4 and at most 8 live slots lie in one aligned block, and exactly 8 in some aligned block of every group.
All inputs are finite; a program needn't handle non-finite values.
Results may differ from the reference program's by a relative error of at most 0.0049.
Values may be sent and summed in bfloat16 or wider, within the bound.
A program may use at most 64 MiB of HBM per device.

```python
import math
import jax
import jax.numpy as jnp
from jax import lax

HQ = 64
KVH = 8
DH = 128
BLOCK = 128
STEPS = 3
Q_DEV = 4
SLOTS = 8
GROUPS = 4
QUERIES = 16
POOL = 64
MAXB = 32
N_BLK = 8


def group_layout(group_key):
    subkeys = jax.random.split(group_key, 9)
    patterns = jnp.array([[8, 8, 6, 4], [8, 6, 6, 6], [7, 7, 6, 6], [8, 7, 7, 4], [8, 8, 5, 5], [7, 7, 8, 4], [8, 6, 7, 5]], jnp.int32)
    quartets = N_BLK // 4
    chosen = jax.random.randint(subkeys[0], (quartets,), 0, 7)
    forced = jnp.array([0, 3, 4], jnp.int32)[jax.random.randint(subkeys[1], (), 0, 3)]
    chosen = chosen.at[0].set(forced)
    device_loads = patterns[chosen].reshape(N_BLK)
    device_loads = device_loads[jax.random.permutation(subkeys[2], N_BLK)]
    slot_ranks = jax.vmap(lambda sub: jax.random.permutation(sub, SLOTS))(jax.random.split(subkeys[3], N_BLK))
    live = (slot_ranks < device_loads[:, None]).reshape(POOL)
    shuffle = jax.random.permutation(subkeys[4], POOL).astype(jnp.int32)
    sort_key = jnp.where(live, shuffle, POOL + shuffle)
    slot_list = jnp.argsort(sort_key, stable=True).astype(jnp.int32)
    longest = MAXB
    rest = 13 * N_BLK // 2 - longest
    first_part = jax.random.randint(subkeys[5], (), 1, rest - 1)
    second_part = jax.random.randint(subkeys[6], (), 1, rest - first_part)
    third_part = rest - first_part - second_part
    pieces = jnp.stack([jnp.array(longest, jnp.int32), first_part, second_part, third_part]).astype(jnp.int32)
    seq_lengths = pieces[jax.random.permutation(subkeys[7], 4)]
    starts = jnp.cumsum(seq_lengths) - seq_lengths
    block_ids = jnp.arange(MAXB, dtype=jnp.int32)
    where_index = jnp.minimum(starts[:, None] + block_ids[None, :], POOL - 1)
    filler = jax.random.randint(subkeys[8], (Q_DEV, MAXB), 0, POOL)
    slot_table = jnp.where(block_ids[None, :] < seq_lengths[:, None], slot_list[where_index], filler)
    return (seq_lengths.astype(jnp.int32), slot_table.astype(jnp.int32))


def layout_all(key):
    group_keys = jax.random.split(jax.random.fold_in(key, 11), GROUPS)
    return jax.vmap(group_layout)(group_keys)


def query_values(key):
    subkey = jax.random.fold_in(key, 23)
    drawn = jnp.clip(jax.random.normal(subkey, (QUERIES * STEPS, HQ * DH), jnp.float32), -6.0, 6.0)
    return drawn


def draw_queries(key, part):
    return query_values(key).astype(jnp.bfloat16)


def draw_lengths(key, part):
    return layout_all(key)[0]


def draw_block_table(key, part):
    return layout_all(key)[1]


def draw_key_pool(key, part):
    subkey = jax.random.fold_in(key, 31)
    pool_shape = (GROUPS, POOL, BLOCK, KVH * DH)
    drawn = jnp.clip(jax.random.normal(subkey, pool_shape, jnp.float32), -6.0, 6.0)
    return drawn.astype(jnp.bfloat16)


def level_of(rng, extent, cuts, smallest, top_value):
    loudness = 1.0
    for dim, blocks in cuts:
        heights = jax.random.uniform(jax.random.fold_in(jax.random.fold_in(rng, 6), dim), (blocks,), jnp.float32, smallest / len(cuts), top_value / len(cuts))
        loudness = loudness * jnp.repeat(jnp.exp(heights), extent[dim] // blocks).reshape((-1,) + (1,) * (len(extent) - 1 - dim))
    return loudness


def scatter_about(stream_key, shape, spread, most, cuts=(), kind=jnp.bfloat16):
    loudness = level_of(stream_key, shape, cuts, -0.22, 0.18) if cuts else 1.0
    entries = jax.random.normal(stream_key, shape, jnp.float32) * spread * loudness
    return jnp.minimum(jnp.maximum(entries, -most), most).astype(kind)


def setup_inputs(seed: int = 0) -> dict:
    key_list = jax.random.split(jax.random.key(seed), 6)
    return {
        "queries": draw_queries(jax.random.fold_in(key_list[5], 71), 0),
        "key_pool": draw_key_pool(jax.random.fold_in(key_list[5], 71), 0),
        "value_pool": scatter_about(key_list[2], (GROUPS, POOL, BLOCK, KVH * DH), 1.0, 6.0, ((0, 4), (1, 8))),
        "lengths": draw_lengths(jax.random.fold_in(key_list[5], 71), 0),
        "block_table": draw_block_table(jax.random.fold_in(key_list[5], 71), 0),
    }


empty_max = -1e+30

def owners(seq_lengths, slot_table, first_slot, slot_count):
    slot_ids = first_slot + jnp.arange(slot_count, dtype=jnp.int32)
    places = jnp.arange(slot_table.shape[1], dtype=jnp.int32)
    in_length = places[None, :] < seq_lengths[:, None]
    matches = (slot_table[:, :, None] == slot_ids[None, None, :]) & in_length[:, :, None]
    return jnp.transpose(jnp.any(matches, axis=1))

def slot_partials(query_block, key_block, value_block):
    slot_count = key_block.shape[0]
    per_group = HQ // KVH
    grouped_q = query_block.reshape(slot_count, STEPS, KVH, per_group, DH)
    grouped_q = jnp.transpose(grouped_q, (0, 2, 1, 3, 4)).reshape(slot_count, KVH, STEPS * per_group, DH).astype(jnp.float32)
    key_heads = key_block.reshape(slot_count, key_block.shape[1], KVH, DH).astype(jnp.float32)
    value_heads = value_block.reshape(slot_count, value_block.shape[1], KVH, DH).astype(jnp.float32)
    scores = jnp.einsum('cgqd,ctgd->cgqt', grouped_q, key_heads) * (1.0 / math.sqrt(DH))
    block_max = lax.optimization_barrier(jnp.max(scores, axis=3))
    weights = jnp.exp(scores - block_max[..., None]).astype(jnp.bfloat16)
    block_total = lax.optimization_barrier(jnp.sum(weights.astype(jnp.float32), axis=3))
    block_out = jnp.einsum('cgqt,ctgd->cgqd', weights.astype(jnp.float32), value_heads)
    return (block_max, block_total, block_out)

def gather_sequences(owned, block_max, block_total, block_out):
    masked = jnp.where(owned[:, :, None, None], block_max[:, None], empty_max)
    seq_max = lax.optimization_barrier(jnp.max(masked, axis=0))
    factor = jnp.where(owned[:, :, None, None], jnp.exp(block_max[:, None] - seq_max[None]), 0.0)
    seq_total = lax.optimization_barrier(jnp.sum(factor * block_total[:, None], axis=0))
    seq_out = jnp.einsum('cqgh,cghd->qghd', factor, block_out, precision=lax.Precision.HIGHEST)
    seq_count = owned.shape[1]
    per_group = HQ // KVH
    seq_max = jnp.transpose(seq_max.reshape(seq_count, KVH, STEPS, per_group), (0, 2, 1, 3)).reshape(seq_count * STEPS, HQ)
    seq_total = jnp.transpose(seq_total.reshape(seq_count, KVH, STEPS, per_group), (0, 2, 1, 3)).reshape(seq_count * STEPS, HQ)
    seq_out = jnp.transpose(seq_out.reshape(seq_count, KVH, STEPS, per_group, DH), (0, 2, 1, 3, 4)).reshape(seq_count * STEPS, HQ, DH)
    return (seq_max, seq_total, seq_out)

def reference(queries, key_pool, value_pool, lengths, block_table):
    grouped = queries.reshape(GROUPS, Q_DEV, STEPS * HQ * DH)

    def one_group(inputs):
        seq_rows, key_rows, value_rows, seq_lengths, slot_table = inputs
        owned = owners(seq_lengths, slot_table, 0, POOL)
        query_block = jnp.dot(owned.astype(jnp.float32), seq_rows.astype(jnp.float32), precision=lax.Precision.HIGHEST).astype(jnp.bfloat16)
        block_max, block_total, block_out = slot_partials(query_block, key_rows, value_rows)
        seq_max, seq_total, seq_out = gather_sequences(owned, block_max, block_total, block_out)
        return (seq_out / seq_total[..., None]).astype(jnp.bfloat16).reshape(Q_DEV * STEPS, HQ * DH)
    attended = lax.map(one_group, (grouped, key_pool, value_pool, lengths, block_table))
    return attended.reshape(QUERIES * STEPS, HQ * DH)
```

```python
import functools
import math

import jax
import jax.numpy as jnp
from jax import lax
from jax.experimental import pallas as pl
from jax.experimental.pallas import tpu as pltpu
from jax.sharding import PartitionSpec as P

HQ = 64
KVH = 8
DH = 128
STEPS = 3


empty_max = -1e30


def owners(seq_lengths, slot_table, first_slot, slot_count):
    slot_ids = first_slot + jnp.arange(slot_count, dtype=jnp.int32)
    places = jnp.arange(slot_table.shape[1], dtype=jnp.int32)
    in_length = places[None, :] < seq_lengths[:, None]
    matches = (slot_table[:, :, None] == slot_ids[None, None, :]) & in_length[:, :, None]
    return jnp.transpose(jnp.any(matches, axis=1))


def slot_partials(query_block, key_block, value_block):
    slot_count = key_block.shape[0]
    per_group = HQ // KVH
    grouped_q = query_block.reshape(slot_count, STEPS, KVH, per_group, DH)
    grouped_q = jnp.transpose(grouped_q, (0, 2, 1, 3, 4)).reshape(
        slot_count, KVH, STEPS * per_group, DH
    )
    key_heads = key_block.reshape(slot_count, key_block.shape[1], KVH, DH)
    value_heads = value_block.reshape(slot_count, value_block.shape[1], KVH, DH)
    scores = jnp.einsum(
        "cgqd,ctgd->cgqt", grouped_q, key_heads, preferred_element_type=jnp.float32
    ) * (1.0 / math.sqrt(DH))
    block_max = jnp.max(scores, axis=3)
    weights = jnp.exp(scores - block_max[..., None]).astype(jnp.bfloat16)
    block_total = jnp.sum(weights.astype(jnp.float32), axis=3)
    block_out = jnp.einsum(
        "cgqt,ctgd->cgqd", weights, value_heads, preferred_element_type=jnp.float32
    )
    return (block_max, block_total, block_out)


def gather_sequences(owned, block_max, block_total, block_out):
    masked = jnp.where(owned[:, :, None, None], block_max[:, None], empty_max)
    seq_max = jnp.max(masked, axis=0)
    factor = jnp.where(owned[:, :, None, None], jnp.exp(block_max[:, None] - seq_max[None]), 0.0)
    seq_total = jnp.sum(factor * block_total[:, None], axis=0)
    seq_out = jnp.einsum("cqgh,cghd->qghd", factor, block_out, precision=lax.Precision.HIGHEST)
    seq_count = owned.shape[1]
    per_group = HQ // KVH
    seq_max = jnp.transpose(
        seq_max.reshape(seq_count, KVH, STEPS, per_group), (0, 2, 1, 3)
    ).reshape(seq_count * STEPS, HQ)
    seq_total = jnp.transpose(
        seq_total.reshape(seq_count, KVH, STEPS, per_group), (0, 2, 1, 3)
    ).reshape(seq_count * STEPS, HQ)
    seq_out = jnp.transpose(
        seq_out.reshape(seq_count, KVH, STEPS, per_group, DH), (0, 2, 1, 3, 4)
    ).reshape(seq_count * STEPS, HQ, DH)
    return (seq_max, seq_total, seq_out)


def block_summary(owned, query_seq, key_block, value_block):
    query_block = jnp.dot(
        owned.astype(jnp.bfloat16), query_seq, preferred_element_type=jnp.float32
    ).astype(jnp.bfloat16)
    block_max, block_total, block_out = slot_partials(query_block, key_block, value_block)
    return gather_sequences(owned, block_max, block_total, block_out)


def body(queries, key_pool, value_pool, lengths, block_table):
    grouped = lax.all_to_all(queries, "grp", split_axis=0, concat_axis=1, tiled=True)
    query_full = lax.all_gather(grouped, "blk", axis=1, tiled=True)
    token_count = query_full.shape[0]
    query_seq = query_full.reshape(token_count // STEPS, STEPS * query_full.shape[1])
    local_keys = key_pool[0]
    local_values = value_pool[0]
    slots_here = local_keys.shape[0]
    first_slot = lax.axis_index("blk") * slots_here
    owned = owners(lengths[0], block_table[0], first_slot, slots_here)
    seq_max, seq_total, seq_out = block_summary(owned, query_seq, local_keys, local_values)
    cycle_size = lax.axis_size("blk")
    heads_here = HQ // cycle_size
    arrived_max, arrived_total, arrived_out = (
        lax.all_to_all(seq_max[None], "blk", split_axis=2, concat_axis=0, tiled=True),
        lax.all_to_all(seq_total[None], "blk", split_axis=2, concat_axis=0, tiled=True),
        lax.all_to_all(seq_out[None], "blk", split_axis=2, concat_axis=0, tiled=True),
    )
    slice_max = jnp.max(arrived_max, axis=0)
    scaling = jnp.exp(arrived_max - slice_max[None])
    mine_total = jnp.sum(scaling * arrived_total, axis=0)
    mine_out = jnp.sum(scaling[..., None] * arrived_out, axis=0)
    attended = (mine_out / mine_total[..., None]).astype(jnp.bfloat16)
    return attended.reshape(mine_out.shape[0], heads_here * DH)


LANES = 128
SUB = 8


def flip(index, step):
    bit = 1
    while bit <= step:
        if step & bit:
            index = index + bit * (1 - 2 * ((index // bit) % 2))
        bit *= 2
    return index


def runs_of(tokens, heads):
    out = []
    for block in range(tokens * heads // SUB):
        row = 0
        while row < SUB:
            head, token = divmod(block * SUB + row, tokens)
            count = min(SUB - row, tokens - token)
            out.append((block, row, head, token, count))
            row += count
    return out


def fused(
    n_blk, n_grp, seqs, tokens, heads, per_group,
    q_hbm, k_hbm, v_hbm, len_hbm, table_hbm, out_ref,
    q_in, q_f32, q_send, q_buf, k_buf, v_buf, q_rows, o_send, o_recv, s_send, s_recv, o_rows,
    table_ref, len_ref, owner_ref, in_sem, kv_sem, z_send, z_recv, p_send, p_recv, o_ssem, o_rsem, s_ssem, s_rsem,
):
    b = lax.axis_index("blk")
    g = lax.axis_index("grp")
    slots = k_hbm.shape[1]
    runs = runs_of(tokens, heads)
    rows_seq = STEPS * per_group
    rows = seqs * rows_seq
    scale = math.log2(math.e) / math.sqrt(DH)

    barrier = pltpu.get_barrier_semaphore()
    for d in range(1, n_grp):
        pl.semaphore_signal(barrier, inc=1, device_id={"grp": flip(g, d)}, device_id_type=pl.DeviceIdType.MESH)
    for r in range(1, n_blk):
        pl.semaphore_signal(barrier, inc=1, device_id={"blk": flip(b, r)}, device_id_type=pl.DeviceIdType.MESH)

    q_copy = pltpu.make_async_copy(q_hbm, q_in, in_sem.at[0])
    table_copy = pltpu.make_async_copy(table_hbm, table_ref, in_sem.at[1])
    len_copy = pltpu.make_async_copy(len_hbm, len_ref, in_sem.at[2])
    q_copy.start()
    table_copy.start()
    len_copy.start()
    kv_copies = []
    for s in range(slots):
        kv_copies.append(pltpu.make_async_copy(k_hbm.at[0, s], k_buf.at[s], kv_sem.at[0, s]))
        kv_copies.append(pltpu.make_async_copy(v_hbm.at[0, s], v_buf.at[s], kv_sem.at[1, s]))

    q_copy.wait()
    for copy in kv_copies:
        copy.start()
    q_f32[...] = q_in[...].astype(jnp.float32)

    def pack(group, store):
        for block in range(tokens * heads // SUB):
            parts = [
                q_f32[group * tokens + t0 : group * tokens + t0 + count, hh * DH : (hh + 1) * DH]
                for (blk_i, _, hh, t0, count) in runs
                if blk_i == block
            ]
            piece = parts[0] if len(parts) == 1 else jnp.concatenate(parts, axis=0)
            store(block, piece.astype(jnp.bfloat16))

    for group in range(n_grp):
        def put(block, piece, group=group):
            q_send[group, block] = piece
        pack(group, put)
    q_buf[0, g] = q_send[g]

    table_copy.wait()
    len_copy.wait()
    table = table_ref[0]
    seq_id = lax.broadcasted_iota(jnp.int32, table.shape, 0)
    place = lax.broadcasted_iota(jnp.int32, table.shape, 1)
    length = jnp.zeros(table.shape, jnp.int32)
    for q in range(seqs):
        length = jnp.where(seq_id == q, jnp.broadcast_to(len_ref[0:1, q : q + 1], table.shape), length)
    o_masks = []
    marked = jnp.where(place < length, table - b * slots, -1)
    for s in range(slots):
        owner = jnp.max(jnp.where(marked == s, seq_id, -1), axis=1, keepdims=True)
        owner = jnp.max(owner, axis=0, keepdims=True)
        o_masks.append(jnp.broadcast_to(owner, (SUB, LANES)))
    owner_ref[...] = jnp.stack(o_masks)

    pl.semaphore_wait(barrier, n_grp - 1 + n_blk - 1)

    def z_copy(d):
        there = flip(g, d)
        return pltpu.make_async_remote_copy(
            src_ref=q_send.at[there], dst_ref=q_buf.at[0, g],
            send_sem=z_send.at[d], recv_sem=z_recv.at[d],
            device_id={"grp": there}, device_id_type=pl.DeviceIdType.MESH,
        )

    def forward(group):
        for r in range(n_blk - 1, 0, -1):
            pltpu.make_async_remote_copy(
                src_ref=q_buf.at[0, group], dst_ref=q_buf.at[r, group],
                send_sem=p_send.at[r], recv_sem=p_recv.at[r],
                device_id={"blk": flip(b, r)}, device_id_type=pl.DeviceIdType.MESH,
            ).start()

    def whole(r):
        return pltpu.make_async_remote_copy(
            src_ref=q_buf.at[0], dst_ref=q_buf.at[r],
            send_sem=p_send.at[r], recv_sem=p_recv.at[r],
            device_id={"blk": flip(b, r)}, device_id_type=pl.DeviceIdType.MESH,
        )

    order = range(1, n_grp)
    z_copies = {d: z_copy(d) for d in order}
    for d in reversed(order):
        z_copies[d].start()
    forward(g)
    for d in order:
        z_copies[d].wait_recv()
        forward(flip(g, d))

    for copy in kv_copies:
        copy.wait()

    def head(r):
        k = flip(b, r)
        lanes = pl.ds(pl.multiple_of(k * DH, DH), DH)
        rows_ref = q_rows.at[r % 2]
        for piece in range(n_grp):
            values = q_buf[r, piece].astype(jnp.float32)
            for block, row, hh, t0, count in runs:
                rows_ref[pl.ds(t0 * per_group + piece * heads + hh, count, stride=per_group), :] = values[
                    block, row : row + count
                ]
        seq_rows = [rows_ref[q * rows_seq : (q + 1) * rows_seq] for q in range(seqs)]
        scores, owned = [], []
        for s in range(slots):
            owner = jnp.concatenate([owner_ref[s]] * (rows_seq // SUB), axis=0)
            owned.append([owner == q for q in range(seqs)])
            mine = seq_rows[0]
            for q in range(1, seqs):
                mine = jnp.where(owned[s][q], seq_rows[q], mine)
            scores.append(
                lax.dot_general(
                    mine.astype(jnp.bfloat16), k_buf[s, :, lanes],
                    (((1,), (1,)), ((), ())), preferred_element_type=jnp.float32,
                )
            )
        tops = []
        for q in range(seqs):
            top = jnp.full((rows_seq, LANES), empty_max, jnp.float32)
            for s in range(slots):
                top = jnp.where(owned[s][q], jnp.maximum(top, scores[s]), top)
            tops.append(jnp.broadcast_to(jnp.max(top, axis=1, keepdims=True) * scale, (rows_seq, LANES)))
        weights = []
        for s in range(slots):
            top = tops[0]
            for q in range(1, seqs):
                top = jnp.where(owned[s][q], tops[q], top)
            weight = jnp.exp2(scores[s] * scale - top)
            weights.append(
                jnp.concatenate(
                    [jnp.where(owned[s][q], weight, 0.0) for q in range(seqs)], axis=0
                ).astype(jnp.bfloat16)
            )
        weights = jnp.concatenate(weights, axis=1)
        values = v_buf[:, :, lanes].reshape(slots * v_buf.shape[1], DH)
        values = jnp.concatenate([values, jnp.ones((values.shape[0], LANES), jnp.bfloat16)], axis=1)
        total = jnp.dot(weights, values, preferred_element_type=jnp.float32)
        return total[:, :DH].astype(jnp.bfloat16), (tops, total[:, DH:])

    def in_rows(tops, total):
        lane = lax.broadcasted_iota(jnp.int32, (rows, LANES), 1)
        stats = jnp.where(lane == 0, jnp.concatenate(tops, axis=0), total)
        stats = jnp.concatenate([stats, jnp.zeros((LANES - rows, LANES), jnp.float32)], axis=0)
        return jnp.transpose(stats)[:SUB]

    def o_copy(r):
        return pltpu.make_async_remote_copy(
            src_ref=o_send.at[r], dst_ref=o_recv.at[r],
            send_sem=o_ssem.at[r], recv_sem=o_rsem.at[r],
            device_id={"blk": flip(b, r)}, device_id_type=pl.DeviceIdType.MESH,
        )

    def s_copy(r):
        return pltpu.make_async_remote_copy(
            src_ref=s_send.at[r], dst_ref=s_recv.at[r],
            send_sem=s_ssem.at[r], recv_sem=s_rsem.at[r],
            device_id={"blk": flip(b, r)}, device_id_type=pl.DeviceIdType.MESH,
        )

    for pair in [(r, r + 1) for r in range(0, n_blk - 2, 2)] + [(n_blk - 2,), (n_blk - 1,)]:
        for r in pair:
            if r:
                whole(r).wait_recv()
        results = [head(r) for r in pair]
        for r, (o, _) in zip(pair, results):
            if r:
                o_send[r] = o
                o_copy(r).start()
            else:
                o_recv[0] = o
        for r, (_, stats) in zip(pair, results):
            if r:
                s_send[r] = in_rows(*stats)
                s_copy(r).start()
            else:
                s_recv[0] = in_rows(*stats)

    for r in range(1, n_blk):
        s_copy(r).wait_recv()
    tops = s_recv[:, 0, :]
    factor = jnp.exp2(tops - jnp.max(tops, axis=0, keepdims=True))
    share = factor / jnp.sum(factor * s_recv[:, 1, :], axis=0, keepdims=True)
    share = jnp.concatenate([share, jnp.zeros((LANES - n_blk, LANES), jnp.float32)], axis=0)
    share = jnp.transpose(share)[:rows]
    merged = jnp.zeros((rows, DH), jnp.float32)
    for r in range(n_blk):
        if r:
            o_copy(r).wait_recv()
        merged = merged + share[:, r : r + 1] * o_recv[r].astype(jnp.float32)
    o_rows[...] = merged
    for h in range(per_group):
        out_ref[:, h * DH : (h + 1) * DH] = o_rows[pl.ds(h, tokens, stride=per_group), :].astype(jnp.bfloat16)

    for d in order:
        z_copies[d].wait_send()
    for r in range(1, n_blk):
        whole(r).wait_send()
        o_copy(r).wait_send()
        s_copy(r).wait_send()


def fused_body(n_blk, n_grp, queries, key_pool, value_pool, lengths, block_table):
    seqs = lengths.shape[1]
    tokens = seqs * STEPS
    heads = queries.shape[1] // DH
    per_group = HQ // KVH
    slots, block = key_pool.shape[1:3]
    rows = tokens * per_group
    blocks = tokens * heads // SUB
    dma = pltpu.SemaphoreType.DMA
    vmem = pl.BlockSpec(memory_space=pltpu.VMEM)
    hbm = pl.BlockSpec(memory_space=pltpu.HBM)
    return pl.pallas_call(
        functools.partial(fused, n_blk, n_grp, seqs, tokens, heads, per_group),
        out_shape=pltpu.VMEM((tokens, per_group * DH), jnp.bfloat16),
        in_specs=[hbm] * 5,
        out_specs=vmem,
        scratch_shapes=[
            pltpu.VMEM(queries.shape, jnp.bfloat16),
            pltpu.VMEM(queries.shape, jnp.float32),
            pltpu.VMEM((n_grp, blocks, SUB, DH), jnp.bfloat16),
            pltpu.VMEM((n_blk, n_grp, blocks, SUB, DH), jnp.bfloat16),
            pltpu.VMEM((slots, block, KVH * DH), jnp.bfloat16),
            pltpu.VMEM((slots, block, KVH * DH), jnp.bfloat16),
            pltpu.VMEM((2, rows, DH), jnp.float32),
            pltpu.VMEM((n_blk, rows, DH), jnp.bfloat16),
            pltpu.VMEM((n_blk, rows, DH), jnp.bfloat16),
            pltpu.VMEM((n_blk, SUB, LANES), jnp.float32),
            pltpu.VMEM((n_blk, SUB, LANES), jnp.float32),
            pltpu.VMEM((rows, DH), jnp.float32),
            pltpu.VMEM(block_table.shape, jnp.int32),
            pltpu.VMEM(lengths.shape, jnp.int32),
            pltpu.VMEM((slots, SUB, LANES), jnp.int32),
            dma((3,)), dma((2, slots)),
            dma((n_grp,)), dma((n_grp,)),
            dma((n_blk,)), dma((n_blk,)),
            dma((n_blk,)), dma((n_blk,)),
            dma((n_blk,)), dma((n_blk,)),
        ],
        compiler_params=pltpu.CompilerParams(
            collective_id=0, has_side_effects=True, vmem_limit_bytes=62914560
        ),
    )(queries, key_pool, value_pool, lengths, block_table)


def choose(mesh):
    n_blk, n_grp = mesh.shape["blk"], mesh.shape["grp"]

    def run(queries, key_pool, value_pool, lengths, block_table):
        rows = lengths.shape[1] * HQ // KVH * STEPS
        fits = (
            n_blk == KVH
            and n_blk & (n_blk - 1) == 0
            and n_grp & (n_grp - 1) == 0
            and queries.shape[1] % DH == 0
            and (lengths.shape[1] * STEPS * queries.shape[1] // DH) % SUB == 0
            and rows % 16 == 0
            and rows <= LANES
            and key_pool.shape[2] == LANES
        )
        if not fits:
            return body(queries, key_pool, value_pool, lengths, block_table)
        return fused_body(n_blk, n_grp, queries, key_pool, value_pool, lengths, block_table)

    return run


def solution(mesh):
    placed = (
        P(None, ("blk", "grp")),
        P("grp", "blk", None, None),
        P("grp", "blk", None, None),
        P("grp", None),
        P("grp", None, None),
    )
    return jax.shard_map(
        choose(mesh), mesh=mesh, in_specs=placed, out_specs=P("grp", "blk"), check_vma=False
    )
```

```python
import functools
import math

import jax
import jax.numpy as jnp
from jax import lax
from jax.experimental import pallas as pl
from jax.experimental.pallas import tpu as pltpu
from jax.sharding import PartitionSpec as P

HQ = 64
KVH = 8
DH = 128
STEPS = 3


empty_max = -1e30


def owners(seq_lengths, slot_table, first_slot, slot_count):
    slot_ids = first_slot + jnp.arange(slot_count, dtype=jnp.int32)
    places = jnp.arange(slot_table.shape[1], dtype=jnp.int32)
    in_length = places[None, :] < seq_lengths[:, None]
    matches = (slot_table[:, :, None] == slot_ids[None, None, :]) & in_length[:, :, None]
    return jnp.transpose(jnp.any(matches, axis=1))


def slot_partials(query_block, key_block, value_block):
    slot_count = key_block.shape[0]
    per_group = HQ // KVH
    grouped_q = query_block.reshape(slot_count, STEPS, KVH, per_group, DH)
    grouped_q = jnp.transpose(grouped_q, (0, 2, 1, 3, 4)).reshape(
        slot_count, KVH, STEPS * per_group, DH
    )
    key_heads = key_block.reshape(slot_count, key_block.shape[1], KVH, DH)
    value_heads = value_block.reshape(slot_count, value_block.shape[1], KVH, DH)
    scores = jnp.einsum(
        "cgqd,ctgd->cgqt", grouped_q, key_heads, preferred_element_type=jnp.float32
    ) * (1.0 / math.sqrt(DH))
    block_max = jnp.max(scores, axis=3)
    weights = jnp.exp(scores - block_max[..., None]).astype(jnp.bfloat16)
    block_total = jnp.sum(weights.astype(jnp.float32), axis=3)
    block_out = jnp.einsum(
        "cgqt,ctgd->cgqd", weights, value_heads, preferred_element_type=jnp.float32
    )
    return (block_max, block_total, block_out)


def gather_sequences(owned, block_max, block_total, block_out):
    masked = jnp.where(owned[:, :, None, None], block_max[:, None], empty_max)
    seq_max = jnp.max(masked, axis=0)
    factor = jnp.where(owned[:, :, None, None], jnp.exp(block_max[:, None] - seq_max[None]), 0.0)
    seq_total = jnp.sum(factor * block_total[:, None], axis=0)
    seq_out = jnp.einsum("cqgh,cghd->qghd", factor, block_out, precision=lax.Precision.HIGHEST)
    seq_count = owned.shape[1]
    per_group = HQ // KVH
    seq_max = jnp.transpose(
        seq_max.reshape(seq_count, KVH, STEPS, per_group), (0, 2, 1, 3)
    ).reshape(seq_count * STEPS, HQ)
    seq_total = jnp.transpose(
        seq_total.reshape(seq_count, KVH, STEPS, per_group), (0, 2, 1, 3)
    ).reshape(seq_count * STEPS, HQ)
    seq_out = jnp.transpose(
        seq_out.reshape(seq_count, KVH, STEPS, per_group, DH), (0, 2, 1, 3, 4)
    ).reshape(seq_count * STEPS, HQ, DH)
    return (seq_max, seq_total, seq_out)


def block_summary(owned, query_seq, key_block, value_block):
    query_block = jnp.dot(
        owned.astype(jnp.bfloat16), query_seq, preferred_element_type=jnp.float32
    ).astype(jnp.bfloat16)
    block_max, block_total, block_out = slot_partials(query_block, key_block, value_block)
    return gather_sequences(owned, block_max, block_total, block_out)


def body(queries, key_pool, value_pool, lengths, block_table):
    grouped = lax.all_to_all(queries, "grp", split_axis=0, concat_axis=1, tiled=True)
    query_full = lax.all_gather(grouped, "blk", axis=1, tiled=True)
    token_count = query_full.shape[0]
    query_seq = query_full.reshape(token_count // STEPS, STEPS * query_full.shape[1])
    local_keys = key_pool[0]
    local_values = value_pool[0]
    slots_here = local_keys.shape[0]
    first_slot = lax.axis_index("blk") * slots_here
    owned = owners(lengths[0], block_table[0], first_slot, slots_here)
    seq_max, seq_total, seq_out = block_summary(owned, query_seq, local_keys, local_values)
    cycle_size = lax.axis_size("blk")
    heads_here = HQ // cycle_size
    arrived_max, arrived_total, arrived_out = (
        lax.all_to_all(seq_max[None], "blk", split_axis=2, concat_axis=0, tiled=True),
        lax.all_to_all(seq_total[None], "blk", split_axis=2, concat_axis=0, tiled=True),
        lax.all_to_all(seq_out[None], "blk", split_axis=2, concat_axis=0, tiled=True),
    )
    slice_max = jnp.max(arrived_max, axis=0)
    scaling = jnp.exp(arrived_max - slice_max[None])
    mine_total = jnp.sum(scaling * arrived_total, axis=0)
    mine_out = jnp.sum(scaling[..., None] * arrived_out, axis=0)
    attended = (mine_out / mine_total[..., None]).astype(jnp.bfloat16)
    return attended.reshape(mine_out.shape[0], heads_here * DH)


LANES = 128
SUB = 8


def flip(index, step):
    bit = 1
    while bit <= step:
        if step & bit:
            index = index + bit * (1 - 2 * ((index // bit) % 2))
        bit *= 2
    return index


def pieces_of(tokens, heads):
    out = []
    for block in range(tokens * heads // SUB):
        row = block * SUB
        parts = []
        while row < (block + 1) * SUB:
            head, token = divmod(row, tokens)
            count = min((block + 1) * SUB - row, tokens - token)
            parts.append((head, token, count))
            row += count
        out.append(parts)
    return out


def fused(
    n_blk, n_grp, seqs, tokens, heads, per_group,
    q_hbm, k_hbm, v_hbm, len_hbm, table_hbm, out_ref,
    q_in, q_f32, q_send, q_buf, k_buf, v_buf, o_send, o_recv, s_send, s_recv, o_rows,
    table_ref, len_ref, bias_ref, in_sem, kv_sem, z_send, z_recv, p_send, p_recv, o_ssem, o_rsem, s_ssem, s_rsem,
):
    b = lax.axis_index("blk")
    g = lax.axis_index("grp")
    slots, block = k_hbm.shape[1:3]
    rows = tokens * per_group
    period = bias_ref.shape[1]
    scale = math.log2(math.e) / math.sqrt(DH)

    q_copy = pltpu.make_async_copy(q_hbm, q_in, in_sem.at[0])
    table_copy = pltpu.make_async_copy(table_hbm, table_ref, in_sem.at[1])
    len_copy = pltpu.make_async_copy(len_hbm, len_ref, in_sem.at[2])
    q_copy.start()
    table_copy.start()
    len_copy.start()
    barrier = pltpu.get_barrier_semaphore()
    for d in range(1, n_grp):
        pl.semaphore_signal(barrier, inc=1, device_id={"grp": flip(g, d)}, device_id_type=pl.DeviceIdType.MESH)
    for r in range(1, n_blk):
        pl.semaphore_signal(barrier, inc=1, device_id={"blk": flip(b, r)}, device_id_type=pl.DeviceIdType.MESH)

    q_copy.wait()
    for k in range(KVH):
        lanes = pl.ds(k * DH, DH)
        pltpu.make_async_copy(k_hbm.at[0, :, :, lanes], k_buf.at[k], kv_sem.at[0]).start()
    for k in range(KVH):
        lanes = pl.ds(k * DH, DH)
        pltpu.make_async_copy(v_hbm.at[0, :, :, lanes], v_buf.at[k], kv_sem.at[1]).start()

    q_f32[...] = q_in[...].astype(jnp.float32)
    for group in range(n_grp):
        for i, parts in enumerate(pieces_of(tokens, heads)):
            parts = [
                q_f32[group * tokens + t0 : group * tokens + t0 + count, hh * DH : (hh + 1) * DH]
                for hh, t0, count in parts
            ]
            piece = parts[0] if len(parts) == 1 else jnp.concatenate(parts, axis=0)
            q_send[group, i] = piece.astype(jnp.bfloat16)
    q_buf[0, g] = q_send[g]

    pl.semaphore_wait(barrier, n_grp - 1 + n_blk - 1)

    def z_copy(d):
        there = flip(g, d)
        return pltpu.make_async_remote_copy(
            src_ref=q_send.at[there], dst_ref=q_buf.at[0, g],
            send_sem=z_send.at[0], recv_sem=z_recv.at[d],
            device_id={"grp": there}, device_id_type=pl.DeviceIdType.MESH,
        )

    def forward(group):
        for r in range(n_blk - 1, 0, -1):
            pltpu.make_async_remote_copy(
                src_ref=q_buf.at[0, group], dst_ref=q_buf.at[r, group],
                send_sem=p_send.at[0], recv_sem=p_recv.at[r // 2],
                device_id={"blk": flip(b, r)}, device_id_type=pl.DeviceIdType.MESH,
            ).start()

    def across(src, dst, send, recv):
        return pltpu.make_async_remote_copy(
            src_ref=src, dst_ref=dst, send_sem=send, recv_sem=recv,
            device_id={"blk": flip(b, 1)}, device_id_type=pl.DeviceIdType.MESH,
        )

    order = range(1, n_grp)
    z_copies = {d: z_copy(d) for d in order}
    for d in reversed(order):
        z_copies[d].start()
    forward(g)

    table_copy.wait()
    len_copy.wait()
    table = table_ref[0]
    seq_id = lax.broadcasted_iota(jnp.int32, table.shape, 0)
    place = lax.broadcasted_iota(jnp.int32, table.shape, 1)
    length = jnp.zeros(table.shape, jnp.int32)
    for q in range(seqs):
        length = jnp.where(seq_id == q, jnp.broadcast_to(len_ref[0:1, q : q + 1], table.shape), length)
    marked = jnp.where(place < length, table - b * slots, -1)
    row_seq = (lax.broadcasted_iota(jnp.int32, (period, LANES), 0) % tokens) // STEPS
    for s in range(slots):
        owner = jnp.max(jnp.where(marked == s, seq_id, -1), axis=1, keepdims=True)
        owner = jnp.max(owner, axis=0, keepdims=True)
        owner = jnp.broadcast_to(owner, (period, LANES))
        bias_ref[s] = jnp.where(owner == row_seq, 0.0, empty_max)

    for d in order:
        z_copies[d].wait_recv()
        forward(flip(g, d))

    for i, buf in enumerate((k_buf, v_buf)):
        pltpu.make_async_copy(buf, buf, kv_sem.at[i]).wait()

    def head_pair(r):
        ks = [flip(b, r), flip(b, r + 1)]
        queries = [
            q_buf[r + i].astype(jnp.float32).reshape(rows, DH).astype(jnp.bfloat16) for i in range(2)
        ]
        blank = jnp.zeros((rows, DH), jnp.bfloat16)
        both = jnp.concatenate(
            [
                jnp.concatenate([queries[0], blank], axis=1),
                jnp.concatenate([blank, queries[1]], axis=1),
            ],
            axis=0,
        )
        step = 2 if slots % 2 == 0 else 1
        scores = []
        for s in range(0, slots, step):
            keys = jnp.concatenate(
                [k_buf[k, s : s + step].reshape(step * block, DH) for k in ks], axis=1
            )
            out = lax.dot_general(
                both, keys, (((1,), (1,)), ((), ())), preferred_element_type=jnp.float32
            )
            scores += [out[:, i * block : (i + 1) * block] for i in range(step)]
        results = []
        for i, k in enumerate(ks):
            mine = []
            for s in range(slots):
                bias = jnp.concatenate([bias_ref[s]] * (rows // period), axis=0)
                mine.append(scores[s][i * rows : (i + 1) * rows] * scale + bias)
            top = mine[0]
            for s in range(1, slots):
                top = jnp.maximum(top, mine[s])
            top = jnp.broadcast_to(jnp.max(top, axis=1, keepdims=True), (rows, LANES))
            weights = jnp.concatenate([jnp.exp2(x - top).astype(jnp.bfloat16) for x in mine], axis=1)
            values = v_buf[k].reshape(slots * block, DH)
            values = jnp.concatenate([values, jnp.ones(values.shape, jnp.bfloat16)], axis=1)
            total = jnp.dot(weights, values, preferred_element_type=jnp.float32)
            results.append((total[:, :DH].astype(jnp.bfloat16), top, total[:, DH:]))
        return results

    def in_rows(results):
        lane = lax.broadcasted_iota(jnp.int32, (rows, LANES), 1)
        stats = jnp.zeros((rows, LANES), jnp.float32)
        for i, (_, top, total) in enumerate(results):
            stats = jnp.where(lane == i * SUB, top, stats)
            stats = jnp.where(lane == i * SUB + 1, total, stats)
        stats = jnp.concatenate([stats, jnp.zeros((LANES - rows, LANES), jnp.float32)], axis=0)
        return jnp.transpose(stats)[: 2 * SUB]

    def o_copy(r):
        return pltpu.make_async_remote_copy(
            src_ref=o_send.at[r], dst_ref=o_recv.at[r],
            send_sem=o_ssem.at[0], recv_sem=o_rsem.at[0],
            device_id={"blk": flip(b, r)}, device_id_type=pl.DeviceIdType.MESH,
        )

    def s_copy(r):
        return pltpu.make_async_remote_copy(
            src_ref=s_send.at[r], dst_ref=s_recv.at[r],
            send_sem=s_ssem.at[0], recv_sem=s_rsem.at[0],
            device_id={"blk": flip(b, r)}, device_id_type=pl.DeviceIdType.MESH,
        )

    def arrived(first):
        low = max(first, 1)
        part = q_buf.at[pl.ds(low, first + 2 - low)]
        across(part, part, p_send.at[0], p_recv.at[first // 2]).wait_recv()

    for first in (0, 2, 4, 6):
        arrived(first)
        results = head_pair(first)
        for i, (o, _, _) in enumerate(results):
            r = first + i
            if r:
                o_send[r] = o
                o_copy(r).start()
            else:
                o_recv[0] = o
        stats = in_rows(results)
        for i in range(2):
            r = first + i
            if r:
                s_send[r] = stats[i * SUB : (i + 1) * SUB]
                s_copy(r).start()
            else:
                s_recv[0] = stats[:SUB]

    others = pl.ds(1, n_blk - 1)
    across(s_recv.at[others], s_recv.at[others], s_ssem.at[0], s_rsem.at[0]).wait_recv()
    tops = s_recv[:, 0, :]
    factor = jnp.exp2(tops - jnp.max(tops, axis=0, keepdims=True))
    share = factor / jnp.sum(factor * s_recv[:, 1, :], axis=0, keepdims=True)
    share = jnp.concatenate([share, jnp.zeros((LANES - n_blk, LANES), jnp.float32)], axis=0)
    share = jnp.transpose(share)[:rows]
    across(o_recv.at[others], o_recv.at[others], o_ssem.at[0], o_rsem.at[0]).wait_recv()
    merged = jnp.zeros((rows, DH), jnp.float32)
    for r in range(n_blk):
        merged = merged + share[:, r : r + 1] * o_recv[r].astype(jnp.float32)
    o_rows[...] = merged
    for h in range(per_group):
        out_ref[:, h * DH : (h + 1) * DH] = o_rows[h * tokens : (h + 1) * tokens, :].astype(jnp.bfloat16)

    z_part = q_buf.at[0, pl.ds(1, n_grp - 1)]
    across(z_part, z_part, z_send.at[0], z_recv.at[0]).wait_send()
    across(q_buf.at[others], q_buf.at[others], p_send.at[0], p_recv.at[0]).wait_send()
    across(o_send.at[others], o_send.at[others], o_ssem.at[0], o_rsem.at[0]).wait_send()
    across(s_send.at[others], s_send.at[others], s_ssem.at[0], s_rsem.at[0]).wait_send()


def fused_body(n_blk, n_grp, queries, key_pool, value_pool, lengths, block_table):
    seqs = lengths.shape[1]
    tokens = seqs * STEPS
    heads = queries.shape[1] // DH
    per_group = HQ // KVH
    slots, block = key_pool.shape[1:3]
    rows = tokens * per_group
    blocks = tokens * heads // SUB
    dma = pltpu.SemaphoreType.DMA
    vmem = pl.BlockSpec(memory_space=pltpu.VMEM)
    hbm = pl.BlockSpec(memory_space=pltpu.HBM)
    return pl.pallas_call(
        functools.partial(fused, n_blk, n_grp, seqs, tokens, heads, per_group),
        out_shape=pltpu.VMEM((tokens, per_group * DH), jnp.bfloat16),
        in_specs=[hbm] * 5,
        out_specs=vmem,
        scratch_shapes=[
            pltpu.VMEM(queries.shape, jnp.bfloat16),
            pltpu.VMEM(queries.shape, jnp.float32),
            pltpu.VMEM((n_grp, blocks, SUB, DH), jnp.bfloat16),
            pltpu.VMEM((n_blk, n_grp, blocks, SUB, DH), jnp.bfloat16),
            pltpu.VMEM((KVH, slots, block, DH), jnp.bfloat16),
            pltpu.VMEM((KVH, slots, block, DH), jnp.bfloat16),
            pltpu.VMEM((n_blk, rows, DH), jnp.bfloat16),
            pltpu.VMEM((n_blk, rows, DH), jnp.bfloat16),
            pltpu.VMEM((n_blk, SUB, LANES), jnp.float32),
            pltpu.VMEM((n_blk, SUB, LANES), jnp.float32),
            pltpu.VMEM((rows, DH), jnp.float32),
            pltpu.VMEM(block_table.shape, jnp.int32),
            pltpu.VMEM(lengths.shape, jnp.int32),
            pltpu.VMEM((slots, math.lcm(tokens, SUB), LANES), jnp.float32),
            dma((3,)), dma((2,)),
            dma((1,)), dma((n_grp,)),
            dma((1,)), dma((n_blk // 2,)),
            dma((1,)), dma((1,)),
            dma((1,)), dma((1,)),
        ],
        compiler_params=pltpu.CompilerParams(
            collective_id=0, has_side_effects=True, vmem_limit_bytes=62914560
        ),
    )(queries, key_pool, value_pool, lengths, block_table)


def choose(mesh):
    n_blk, n_grp = mesh.shape["blk"], mesh.shape["grp"]

    def run(queries, key_pool, value_pool, lengths, block_table):
        rows = lengths.shape[1] * HQ // KVH * STEPS
        fits = (
            n_blk == KVH
            and n_blk & (n_blk - 1) == 0
            and n_grp & (n_grp - 1) == 0
            and queries.shape[1] % DH == 0
            and (lengths.shape[1] * STEPS * queries.shape[1] // DH) % SUB == 0
            and rows % math.lcm(lengths.shape[1] * STEPS, SUB) == 0
            and rows % 16 == 0
            and rows <= LANES
            and key_pool.shape[2] == LANES
        )
        if not fits:
            return body(queries, key_pool, value_pool, lengths, block_table)
        return fused_body(n_blk, n_grp, queries, key_pool, value_pool, lengths, block_table)

    return run


def solution(mesh):
    placed = (
        P(None, ("blk", "grp")),
        P("grp", "blk", None, None),
        P("grp", "blk", None, None),
        P("grp", None),
        P("grp", None, None),
    )
    return jax.shard_map(
        choose(mesh), mesh=mesh, in_specs=placed, out_specs=P("grp", "blk"), check_vma=False
    )
```

```python
import functools
import math

import jax
import jax.numpy as jnp
from jax import lax
from jax.experimental import pallas as pl
from jax.experimental.pallas import tpu as pltpu
from jax.sharding import PartitionSpec as P

HQ = 64
KVH = 8
DH = 128
STEPS = 3


empty_max = -1e30


def owners(seq_lengths, slot_table, first_slot, slot_count):
    slot_ids = first_slot + jnp.arange(slot_count, dtype=jnp.int32)
    places = jnp.arange(slot_table.shape[1], dtype=jnp.int32)
    in_length = places[None, :] < seq_lengths[:, None]
    matches = (slot_table[:, :, None] == slot_ids[None, None, :]) & in_length[:, :, None]
    return jnp.transpose(jnp.any(matches, axis=1))


def slot_partials(query_block, key_block, value_block):
    slot_count = key_block.shape[0]
    per_group = HQ // KVH
    grouped_q = query_block.reshape(slot_count, STEPS, KVH, per_group, DH)
    grouped_q = jnp.transpose(grouped_q, (0, 2, 1, 3, 4)).reshape(
        slot_count, KVH, STEPS * per_group, DH
    )
    key_heads = key_block.reshape(slot_count, key_block.shape[1], KVH, DH)
    value_heads = value_block.reshape(slot_count, value_block.shape[1], KVH, DH)
    scores = jnp.einsum(
        "cgqd,ctgd->cgqt", grouped_q, key_heads, preferred_element_type=jnp.float32
    ) * (1.0 / math.sqrt(DH))
    block_max = jnp.max(scores, axis=3)
    weights = jnp.exp(scores - block_max[..., None]).astype(jnp.bfloat16)
    block_total = jnp.sum(weights.astype(jnp.float32), axis=3)
    block_out = jnp.einsum(
        "cgqt,ctgd->cgqd", weights, value_heads, preferred_element_type=jnp.float32
    )
    return (block_max, block_total, block_out)


def gather_sequences(owned, block_max, block_total, block_out):
    masked = jnp.where(owned[:, :, None, None], block_max[:, None], empty_max)
    seq_max = jnp.max(masked, axis=0)
    factor = jnp.where(owned[:, :, None, None], jnp.exp(block_max[:, None] - seq_max[None]), 0.0)
    seq_total = jnp.sum(factor * block_total[:, None], axis=0)
    seq_out = jnp.einsum("cqgh,cghd->qghd", factor, block_out, precision=lax.Precision.HIGHEST)
    seq_count = owned.shape[1]
    per_group = HQ // KVH
    seq_max = jnp.transpose(
        seq_max.reshape(seq_count, KVH, STEPS, per_group), (0, 2, 1, 3)
    ).reshape(seq_count * STEPS, HQ)
    seq_total = jnp.transpose(
        seq_total.reshape(seq_count, KVH, STEPS, per_group), (0, 2, 1, 3)
    ).reshape(seq_count * STEPS, HQ)
    seq_out = jnp.transpose(
        seq_out.reshape(seq_count, KVH, STEPS, per_group, DH), (0, 2, 1, 3, 4)
    ).reshape(seq_count * STEPS, HQ, DH)
    return (seq_max, seq_total, seq_out)


def block_summary(owned, query_seq, key_block, value_block):
    query_block = jnp.dot(
        owned.astype(jnp.bfloat16), query_seq, preferred_element_type=jnp.float32
    ).astype(jnp.bfloat16)
    block_max, block_total, block_out = slot_partials(query_block, key_block, value_block)
    return gather_sequences(owned, block_max, block_total, block_out)


def body(queries, key_pool, value_pool, lengths, block_table):
    grouped = lax.all_to_all(queries, "grp", split_axis=0, concat_axis=1, tiled=True)
    query_full = lax.all_gather(grouped, "blk", axis=1, tiled=True)
    token_count = query_full.shape[0]
    query_seq = query_full.reshape(token_count // STEPS, STEPS * query_full.shape[1])
    local_keys = key_pool[0]
    local_values = value_pool[0]
    slots_here = local_keys.shape[0]
    first_slot = lax.axis_index("blk") * slots_here
    owned = owners(lengths[0], block_table[0], first_slot, slots_here)
    seq_max, seq_total, seq_out = block_summary(owned, query_seq, local_keys, local_values)
    cycle_size = lax.axis_size("blk")
    heads_here = HQ // cycle_size
    arrived_max, arrived_total, arrived_out = (
        lax.all_to_all(seq_max[None], "blk", split_axis=2, concat_axis=0, tiled=True),
        lax.all_to_all(seq_total[None], "blk", split_axis=2, concat_axis=0, tiled=True),
        lax.all_to_all(seq_out[None], "blk", split_axis=2, concat_axis=0, tiled=True),
    )
    slice_max = jnp.max(arrived_max, axis=0)
    scaling = jnp.exp(arrived_max - slice_max[None])
    mine_total = jnp.sum(scaling * arrived_total, axis=0)
    mine_out = jnp.sum(scaling[..., None] * arrived_out, axis=0)
    attended = (mine_out / mine_total[..., None]).astype(jnp.bfloat16)
    return attended.reshape(mine_out.shape[0], heads_here * DH)


LANES = 128
SUB = 8


def flip(index, step):
    bit = 1
    while bit <= step:
        if step & bit:
            index = index + bit * (1 - 2 * ((index // bit) % 2))
        bit *= 2
    return index


def pieces_of(tokens, heads):
    out = []
    for block in range(tokens * heads // SUB):
        row = block * SUB
        parts = []
        while row < (block + 1) * SUB:
            head, token = divmod(row, tokens)
            count = min((block + 1) * SUB - row, tokens - token)
            parts.append((head, token, count))
            row += count
        out.append(parts)
    return out


def fused(
    n_blk, n_grp, seqs, tokens, heads, per_group,
    q_hbm, k_hbm, v_hbm, len_hbm, table_hbm, out_ref,
    q_in, q_f32, q_send, q_buf, k_buf, v_buf, o_send, o_recv, s_send, s_recv, o_rows,
    table_ref, len_ref, bias_ref, in_sem, kv_sem, z_send, z_recv, p_send, p_recv, d_send, o_ssem, o_rsem, s_ssem, s_rsem, ready,
):
    b = lax.axis_index("blk")
    g = lax.axis_index("grp")
    slots, block = k_hbm.shape[1:3]
    rows = tokens * per_group
    period = bias_ref.shape[1]
    scale = math.log2(math.e) / math.sqrt(DH)

    q_copy = pltpu.make_async_copy(q_hbm, q_in, in_sem.at[0])
    table_copy = pltpu.make_async_copy(table_hbm, table_ref, in_sem.at[1])
    len_copy = pltpu.make_async_copy(len_hbm, len_ref, in_sem.at[2])
    q_copy.start()
    table_copy.start()
    len_copy.start()
    barrier = pltpu.get_barrier_semaphore()
    side, up = n_blk // 4, n_blk // 2
    near = [r for r in range(1, n_blk) if not (r & side and r & up)]
    for d in range(1, n_grp):
        pl.semaphore_signal(barrier, inc=1, device_id={"grp": flip(g, d)}, device_id_type=pl.DeviceIdType.MESH)
    for r in near:
        pl.semaphore_signal(barrier, inc=1, device_id={"blk": flip(b, r)}, device_id_type=pl.DeviceIdType.MESH)

    @pl.when(g == 0)
    def _():
        for r in range(1, n_blk):
            pl.semaphore_signal(
                barrier, inc=1, device_id={"blk": flip(b, r), "grp": n_grp - 1},
                device_id_type=pl.DeviceIdType.MESH,
            )

    q_copy.wait()
    for k in range(KVH):
        lanes = pl.ds(k * DH, DH)
        pltpu.make_async_copy(k_hbm.at[0, :, :, lanes], k_buf.at[k], kv_sem.at[0]).start()
    for k in range(KVH):
        lanes = pl.ds(k * DH, DH)
        pltpu.make_async_copy(v_hbm.at[0, :, :, lanes], v_buf.at[k], kv_sem.at[1]).start()

    q_f32[...] = q_in[...].astype(jnp.float32)
    for group in range(n_grp):
        for i, parts in enumerate(pieces_of(tokens, heads)):
            parts = [
                q_f32[group * tokens + t0 : group * tokens + t0 + count, hh * DH : (hh + 1) * DH]
                for hh, t0, count in parts
            ]
            piece = parts[0] if len(parts) == 1 else jnp.concatenate(parts, axis=0)
            q_send[group, i] = piece.astype(jnp.bfloat16)
    q_buf[0, g] = q_send[g]

    pl.semaphore_wait(barrier, n_grp - 1 + len(near) + g // (n_grp - 1) * (n_blk - 1))

    def z_copy(d):
        there = flip(g, d)
        return pltpu.make_async_remote_copy(
            src_ref=q_send.at[there], dst_ref=q_buf.at[0, g],
            send_sem=z_send.at[0], recv_sem=z_recv.at[d],
            device_id={"grp": there}, device_id_type=pl.DeviceIdType.MESH,
        )

    def forward(group, targets=tuple(range(n_blk - 1, 0, -1))):
        for r in targets:
            pltpu.make_async_remote_copy(
                src_ref=q_buf.at[0, group], dst_ref=q_buf.at[r, group],
                send_sem=p_send.at[0], recv_sem=p_recv.at[r],
                device_id={"blk": flip(b, r)}, device_id_type=pl.DeviceIdType.MESH,
            ).start()

    def across(src, dst, send, recv):
        return pltpu.make_async_remote_copy(
            src_ref=src, dst_ref=dst, send_sem=send, recv_sem=recv,
            device_id={"blk": flip(b, 1)}, device_id_type=pl.DeviceIdType.MESH,
        )

    order = range(1, n_grp)
    z_copies = {d: z_copy(d) for d in order}
    far = n_grp - 1
    for d in reversed(order[:-1]):
        z_copies[d].start()

    @pl.when(g == far)
    def _():
        for r in reversed(range(n_blk)):
            pltpu.make_async_remote_copy(
                src_ref=q_send.at[0], dst_ref=q_buf.at[r, g],
                send_sem=d_send.at[0], recv_sem=p_recv.at[r] if r else z_recv.at[far],
                device_id={"blk": flip(b, r), "grp": 0}, device_id_type=pl.DeviceIdType.MESH,
            ).start()

    @pl.when(g != far)
    def _():
        z_copies[far].start()

    pl.semaphore_signal(ready, inc=1, device_id={"blk": flip(b, side)}, device_id_type=pl.DeviceIdType.MESH)
    forward(g, near)

    table_copy.wait()
    len_copy.wait()
    table = table_ref[0]
    seq_id = lax.broadcasted_iota(jnp.int32, table.shape, 0)
    place = lax.broadcasted_iota(jnp.int32, table.shape, 1)
    length = jnp.zeros(table.shape, jnp.int32)
    for q in range(seqs):
        length = jnp.where(seq_id == q, jnp.broadcast_to(len_ref[0:1, q : q + 1], table.shape), length)
    marked = jnp.where(place < length, table - b * slots, -1)
    row_seq = (lax.broadcasted_iota(jnp.int32, (period, LANES), 0) % tokens) // STEPS
    for s in range(slots):
        owner = jnp.max(jnp.where(marked == s, seq_id, -1), axis=1, keepdims=True)
        owner = jnp.max(owner, axis=0, keepdims=True)
        owner = jnp.broadcast_to(owner, (period, LANES))
        bias_ref[s] = jnp.where(owner == row_seq, 0.0, empty_max)

    pl.semaphore_wait(ready, 1)
    forward(g, [r for r in range(1, n_blk) if r not in near])
    for d in order:
        z_copies[d].wait_recv()
        if d < far:
            forward(flip(g, d))

    @pl.when(g > 0)
    def _():
        forward(flip(g, far))

    for i, buf in enumerate((k_buf, v_buf)):
        pltpu.make_async_copy(buf, buf, kv_sem.at[i]).wait()

    def head_pair(pair):
        ks = [flip(b, r) for r in pair]
        queries = [
            q_buf[r].astype(jnp.float32).reshape(rows, DH).astype(jnp.bfloat16) for r in pair
        ]
        blank = jnp.zeros((rows, DH), jnp.bfloat16)
        both = jnp.concatenate(
            [
                jnp.concatenate([queries[0], blank], axis=1),
                jnp.concatenate([blank, queries[1]], axis=1),
            ],
            axis=0,
        )
        step = 2 if slots % 2 == 0 else 1
        scores = []
        for s in range(0, slots, step):
            keys = jnp.concatenate(
                [k_buf[k, s : s + step].reshape(step * block, DH) for k in ks], axis=1
            )
            out = lax.dot_general(
                both, keys, (((1,), (1,)), ((), ())), preferred_element_type=jnp.float32
            )
            scores += [out[:, i * block : (i + 1) * block] for i in range(step)]
        results = []
        for i, k in enumerate(ks):
            mine = []
            for s in range(slots):
                bias = jnp.concatenate([bias_ref[s]] * (rows // period), axis=0)
                mine.append(scores[s][i * rows : (i + 1) * rows] * scale + bias)
            top = mine[0]
            for s in range(1, slots):
                top = jnp.maximum(top, mine[s])
            top = jnp.broadcast_to(jnp.max(top, axis=1, keepdims=True), (rows, LANES))
            weights = jnp.concatenate([jnp.exp2(x - top).astype(jnp.bfloat16) for x in mine], axis=1)
            values = v_buf[k].reshape(slots * block, DH)
            values = jnp.concatenate([values, jnp.ones(values.shape, jnp.bfloat16)], axis=1)
            total = jnp.dot(weights, values, preferred_element_type=jnp.float32)
            results.append((total[:, :DH].astype(jnp.bfloat16), top, total[:, DH:]))
        return results

    def in_rows(results):
        lane = lax.broadcasted_iota(jnp.int32, (rows, LANES), 1)
        stats = jnp.zeros((rows, LANES), jnp.float32)
        for i, (_, top, total) in enumerate(results):
            stats = jnp.where(lane == i * SUB, top, stats)
            stats = jnp.where(lane == i * SUB + 1, total, stats)
        stats = jnp.concatenate([stats, jnp.zeros((LANES - rows, LANES), jnp.float32)], axis=0)
        return jnp.transpose(stats)[: 2 * SUB]

    def o_copy(r):
        return pltpu.make_async_remote_copy(
            src_ref=o_send.at[r], dst_ref=o_recv.at[r],
            send_sem=o_ssem.at[0], recv_sem=o_rsem.at[0],
            device_id={"blk": flip(b, r)}, device_id_type=pl.DeviceIdType.MESH,
        )

    def s_copy(r):
        return pltpu.make_async_remote_copy(
            src_ref=s_send.at[r], dst_ref=s_recv.at[r],
            send_sem=s_ssem.at[0], recv_sem=s_rsem.at[0],
            device_id={"blk": flip(b, r)}, device_id_type=pl.DeviceIdType.MESH,
        )

    def arrived(pair):
        for r in pair:
            if r:
                across(q_buf.at[r], q_buf.at[r], p_send.at[0], p_recv.at[r]).wait_recv()

    for pair in ((0,1),(2,4),(6,7),(3,5)):
        arrived(pair)
        results = head_pair(pair)
        for r, (o, _, _) in zip(pair, results):
            if r:
                o_send[r] = o
                o_copy(r).start()
            else:
                o_recv[0] = o
        stats = in_rows(results)
        for i, r in enumerate(pair):
            if r:
                s_send[r] = stats[i * SUB : i * SUB + 2]
                s_copy(r).start()
            else:
                s_recv[0] = stats[:2]

    others = pl.ds(1, n_blk - 1)
    across(s_recv.at[others], s_recv.at[others], s_ssem.at[0], s_rsem.at[0]).wait_recv()
    tops = s_recv[:, 0, :]
    factor = jnp.exp2(tops - jnp.max(tops, axis=0, keepdims=True))
    share = factor / jnp.sum(factor * s_recv[:, 1, :], axis=0, keepdims=True)
    share = jnp.concatenate([share, jnp.zeros((LANES - n_blk, LANES), jnp.float32)], axis=0)
    share = jnp.transpose(share)[:rows]
    across(o_recv.at[others], o_recv.at[others], o_ssem.at[0], o_rsem.at[0]).wait_recv()
    merged = jnp.zeros((rows, DH), jnp.float32)
    for r in range(n_blk):
        merged = merged + share[:, r : r + 1] * o_recv[r].astype(jnp.float32)
    o_rows[...] = merged
    for h in range(per_group):
        out_ref[:, h * DH : (h + 1) * DH] = o_rows[h * tokens : (h + 1) * tokens, :].astype(jnp.bfloat16)

    def sent(part, sem):
        across(part, part, sem, p_recv.at[0]).wait_send()

    @pl.when(g == far)
    def _():
        sent(q_buf.at[0, pl.ds(1, n_grp - 2)], z_send.at[0])
        sent(q_buf.at[:, 0], d_send.at[0])

    @pl.when(g != far)
    def _():
        sent(q_buf.at[0, pl.ds(1, n_grp - 1)], z_send.at[0])

    @pl.when(g == 0)
    def _():
        sent(q_buf.at[others, pl.ds(1, n_grp - 1)], p_send.at[0])

    @pl.when(g > 0)
    def _():
        sent(q_buf.at[others], p_send.at[0])

    across(o_send.at[others], o_send.at[others], o_ssem.at[0], o_rsem.at[0]).wait_send()
    across(s_send.at[others], s_send.at[others], s_ssem.at[0], s_rsem.at[0]).wait_send()


def fused_body(n_blk, n_grp, queries, key_pool, value_pool, lengths, block_table):
    seqs = lengths.shape[1]
    tokens = seqs * STEPS
    heads = queries.shape[1] // DH
    per_group = HQ // KVH
    slots, block = key_pool.shape[1:3]
    rows = tokens * per_group
    blocks = tokens * heads // SUB
    dma = pltpu.SemaphoreType.DMA
    vmem = pl.BlockSpec(memory_space=pltpu.VMEM)
    hbm = pl.BlockSpec(memory_space=pltpu.HBM)
    return pl.pallas_call(
        functools.partial(fused, n_blk, n_grp, seqs, tokens, heads, per_group),
        out_shape=pltpu.VMEM((tokens, per_group * DH), jnp.bfloat16),
        in_specs=[hbm] * 5,
        out_specs=vmem,
        scratch_shapes=[
            pltpu.VMEM(queries.shape, jnp.bfloat16),
            pltpu.VMEM(queries.shape, jnp.float32),
            pltpu.VMEM((n_grp, blocks, SUB, DH), jnp.bfloat16),
            pltpu.VMEM((n_blk, n_grp, blocks, SUB, DH), jnp.bfloat16),
            pltpu.VMEM((KVH, slots, block, DH), jnp.bfloat16),
            pltpu.VMEM((KVH, slots, block, DH), jnp.bfloat16),
            pltpu.VMEM((n_blk, rows, DH), jnp.bfloat16),
            pltpu.VMEM((n_blk, rows, DH), jnp.bfloat16),
            pltpu.VMEM((n_blk, 2, LANES), jnp.float32),
            pltpu.VMEM((n_blk, 2, LANES), jnp.float32),
            pltpu.VMEM((rows, DH), jnp.float32),
            pltpu.VMEM(block_table.shape, jnp.int32),
            pltpu.VMEM(lengths.shape, jnp.int32),
            pltpu.VMEM((slots, math.lcm(tokens, SUB), LANES), jnp.float32),
            dma((3,)), dma((2,)),
            dma((1,)), dma((n_grp,)),
            dma((1,)), dma((n_blk,)), dma((1,)),
            dma((1,)), dma((1,)),
            dma((1,)), dma((1,)), pltpu.SemaphoreType.REGULAR,
        ],
        compiler_params=pltpu.CompilerParams(
            collective_id=0, has_side_effects=True, vmem_limit_bytes=62914560
        ),
    )(queries, key_pool, value_pool, lengths, block_table)


def choose(mesh):
    n_blk, n_grp = mesh.shape["blk"], mesh.shape["grp"]

    def run(queries, key_pool, value_pool, lengths, block_table):
        rows = lengths.shape[1] * HQ // KVH * STEPS
        fits = (
            n_blk == KVH
            and n_blk & (n_blk - 1) == 0
            and n_grp & (n_grp - 1) == 0
            and queries.shape[1] % DH == 0
            and (lengths.shape[1] * STEPS * queries.shape[1] // DH) % SUB == 0
            and rows % math.lcm(lengths.shape[1] * STEPS, SUB) == 0
            and rows % 16 == 0
            and rows <= LANES
            and key_pool.shape[2] == LANES
        )
        if not fits:
            return body(queries, key_pool, value_pool, lengths, block_table)
        return fused_body(n_blk, n_grp, queries, key_pool, value_pool, lengths, block_table)

    return run


def solution(mesh):
    placed = (
        P(None, ("blk", "grp")),
        P("grp", "blk", None, None),
        P("grp", "blk", None, None),
        P("grp", None),
        P("grp", None, None),
    )
    return jax.shard_map(
        choose(mesh), mesh=mesh, in_specs=placed, out_specs=P("grp", "blk"), check_vma=False
    )
```

```python
import functools
import math

import jax
import jax.numpy as jnp
from jax import lax
from jax.experimental import pallas as pl
from jax.experimental.pallas import tpu as pltpu
from jax.sharding import PartitionSpec as P

HQ = 64
KVH = 8
DH = 128
STEPS = 3


empty_max = -1e30


def owners(seq_lengths, slot_table, first_slot, slot_count):
    slot_ids = first_slot + jnp.arange(slot_count, dtype=jnp.int32)
    places = jnp.arange(slot_table.shape[1], dtype=jnp.int32)
    in_length = places[None, :] < seq_lengths[:, None]
    matches = (slot_table[:, :, None] == slot_ids[None, None, :]) & in_length[:, :, None]
    return jnp.transpose(jnp.any(matches, axis=1))


def slot_partials(query_block, key_block, value_block):
    slot_count = key_block.shape[0]
    per_group = HQ // KVH
    grouped_q = query_block.reshape(slot_count, STEPS, KVH, per_group, DH)
    grouped_q = jnp.transpose(grouped_q, (0, 2, 1, 3, 4)).reshape(
        slot_count, KVH, STEPS * per_group, DH
    )
    key_heads = key_block.reshape(slot_count, key_block.shape[1], KVH, DH)
    value_heads = value_block.reshape(slot_count, value_block.shape[1], KVH, DH)
    scores = jnp.einsum(
        "cgqd,ctgd->cgqt", grouped_q, key_heads, preferred_element_type=jnp.float32
    ) * (1.0 / math.sqrt(DH))
    block_max = jnp.max(scores, axis=3)
    weights = jnp.exp(scores - block_max[..., None]).astype(jnp.bfloat16)
    block_total = jnp.sum(weights.astype(jnp.float32), axis=3)
    block_out = jnp.einsum(
        "cgqt,ctgd->cgqd", weights, value_heads, preferred_element_type=jnp.float32
    )
    return (block_max, block_total, block_out)


def gather_sequences(owned, block_max, block_total, block_out):
    masked = jnp.where(owned[:, :, None, None], block_max[:, None], empty_max)
    seq_max = jnp.max(masked, axis=0)
    factor = jnp.where(owned[:, :, None, None], jnp.exp(block_max[:, None] - seq_max[None]), 0.0)
    seq_total = jnp.sum(factor * block_total[:, None], axis=0)
    seq_out = jnp.einsum("cqgh,cghd->qghd", factor, block_out, precision=lax.Precision.HIGHEST)
    seq_count = owned.shape[1]
    per_group = HQ // KVH
    seq_max = jnp.transpose(
        seq_max.reshape(seq_count, KVH, STEPS, per_group), (0, 2, 1, 3)
    ).reshape(seq_count * STEPS, HQ)
    seq_total = jnp.transpose(
        seq_total.reshape(seq_count, KVH, STEPS, per_group), (0, 2, 1, 3)
    ).reshape(seq_count * STEPS, HQ)
    seq_out = jnp.transpose(
        seq_out.reshape(seq_count, KVH, STEPS, per_group, DH), (0, 2, 1, 3, 4)
    ).reshape(seq_count * STEPS, HQ, DH)
    return (seq_max, seq_total, seq_out)


def block_summary(owned, query_seq, key_block, value_block):
    query_block = jnp.dot(
        owned.astype(jnp.bfloat16), query_seq, preferred_element_type=jnp.float32
    ).astype(jnp.bfloat16)
    block_max, block_total, block_out = slot_partials(query_block, key_block, value_block)
    return gather_sequences(owned, block_max, block_total, block_out)


def body(queries, key_pool, value_pool, lengths, block_table):
    grouped = lax.all_to_all(queries, "grp", split_axis=0, concat_axis=1, tiled=True)
    query_full = lax.all_gather(grouped, "blk", axis=1, tiled=True)
    token_count = query_full.shape[0]
    query_seq = query_full.reshape(token_count // STEPS, STEPS * query_full.shape[1])
    local_keys = key_pool[0]
    local_values = value_pool[0]
    slots_here = local_keys.shape[0]
    first_slot = lax.axis_index("blk") * slots_here
    owned = owners(lengths[0], block_table[0], first_slot, slots_here)
    seq_max, seq_total, seq_out = block_summary(owned, query_seq, local_keys, local_values)
    cycle_size = lax.axis_size("blk")
    heads_here = HQ // cycle_size
    arrived_max, arrived_total, arrived_out = (
        lax.all_to_all(seq_max[None], "blk", split_axis=2, concat_axis=0, tiled=True),
        lax.all_to_all(seq_total[None], "blk", split_axis=2, concat_axis=0, tiled=True),
        lax.all_to_all(seq_out[None], "blk", split_axis=2, concat_axis=0, tiled=True),
    )
    slice_max = jnp.max(arrived_max, axis=0)
    scaling = jnp.exp(arrived_max - slice_max[None])
    mine_total = jnp.sum(scaling * arrived_total, axis=0)
    mine_out = jnp.sum(scaling[..., None] * arrived_out, axis=0)
    attended = (mine_out / mine_total[..., None]).astype(jnp.bfloat16)
    return attended.reshape(mine_out.shape[0], heads_here * DH)


LANES = 128
SUB = 8


def flip(index, step):
    bit = 1
    while bit <= step:
        if step & bit:
            index = index + bit * (1 - 2 * ((index // bit) % 2))
        bit *= 2
    return index


def pieces_of(tokens, heads):
    out = []
    for block in range(tokens * heads // SUB):
        row = block * SUB
        parts = []
        while row < (block + 1) * SUB:
            head, token = divmod(row, tokens)
            count = min((block + 1) * SUB - row, tokens - token)
            parts.append((head, token, count))
            row += count
        out.append(parts)
    return out


def fused(
    n_blk, n_grp, seqs, tokens, heads, per_group,
    q_hbm, k_hbm, v_hbm, len_hbm, table_hbm, out_ref,
    q_in, q_f32, q_send, q_own, q_buf, k_buf, v_buf, o_send, o_recv, s_send, s_recv, o_rows,
    table_ref, len_ref, bias_ref, in_sem, kv_sem, kv_send, kv_recv,
    z_send, z_recv, p_send, p_recv, d_send, o_ssem, o_rsem, s_ssem, s_rsem,
):
    b = lax.axis_index("blk")
    g = lax.axis_index("grp")
    slots, block = k_hbm.shape[1:3]
    rows = tokens * per_group
    period = bias_ref.shape[1]
    scale = math.log2(math.e) / math.sqrt(DH)
    core = b % 2
    units = n_blk // 2
    peers = [2 * x + 1 for x in range(units)]
    direct = [d for d in (3,) if d < n_grp]
    here = pl.ds(core * slots, slots)

    def signal(device):
        pl.semaphore_signal(barrier, inc=1, device_id=device, device_id_type=pl.DeviceIdType.MESH)

    def remote(src, dst, send, recv, device):
        return pltpu.make_async_remote_copy(
            src_ref=src, dst_ref=dst, send_sem=send, recv_sem=recv,
            device_id=device, device_id_type=pl.DeviceIdType.MESH,
        )

    def like(part, send, recv):
        return remote(part, part, send, recv, {"blk": flip(b, 1)})

    q_copy = pltpu.make_async_copy(q_hbm, q_in, in_sem.at[0])
    table_copy = pltpu.make_async_copy(table_hbm, table_ref, in_sem.at[1])
    len_copy = pltpu.make_async_copy(len_hbm, len_ref, in_sem.at[2])
    q_copy.start()
    table_copy.start()
    len_copy.start()
    barrier = pltpu.get_barrier_semaphore()
    plane = sorted({1, *peers} - {0})
    cross = [r for r in peers if r]
    for d in range(1, n_grp):
        signal({"grp": flip(g, d)})
    for r in plane:
        signal({"blk": flip(b, r)})

    @pl.when(g == 0)
    def _():
        for d in direct:
            for r in cross:
                signal({"blk": flip(b, r), "grp": d})

    q_copy.wait()
    sources = ((k_hbm, k_buf), (v_hbm, v_buf))

    def lanes(r):
        return pl.ds(pl.multiple_of(flip(b, r) * DH, DH), DH)

    for i, (src, dst) in enumerate(sources):
        for x, r in enumerate(peers):
            pltpu.make_async_copy(src.at[0, :, :, lanes(r)], dst.at[x, here], kv_sem.at[i]).start()

    q_f32[...] = q_in[...].astype(jnp.float32)
    for group in range(n_grp):
        for i, parts in enumerate(pieces_of(tokens, heads)):
            parts = [
                q_f32[group * tokens + t0 : group * tokens + t0 + count, hh * DH : (hh + 1) * DH]
                for hh, t0, count in parts
            ]
            piece = parts[0] if len(parts) == 1 else jnp.concatenate(parts, axis=0)
            q_send[group, i] = piece.astype(jnp.bfloat16)
    q_own[g] = q_send[g]

    crossed = 0
    for d in direct:
        crossed = crossed + (1 - jnp.minimum(jnp.abs(g - d), 1)) * len(cross)
    pl.semaphore_wait(barrier, n_grp - 1 + len(plane) + crossed)

    order = range(1, n_grp)

    def z_copy(d):
        there = flip(g, d)
        return remote(q_send.at[there], q_own.at[g], z_send.at[d], z_recv.at[d], {"grp": there})

    def forward(group):
        for r in reversed(peers):
            if r:
                remote(
                    q_own.at[group], q_buf.at[r // 2, group], p_send.at[0], p_recv.at[r // 2],
                    {"blk": flip(b, r)},
                ).start()

    for d in reversed(order):
        if d in direct:
            pl.when(g != d)(z_copy(d).start)
        else:
            z_copy(d).start()
    for d in direct:
        @pl.when(g == d)
        def _(d=d):
            for r in reversed(cross):
                remote(
                    q_send.at[0], q_buf.at[r // 2, g], d_send.at[0], p_recv.at[r // 2],
                    {"blk": flip(b, r), "grp": 0},
                ).start()
    forward(g)

    for i, (src, dst) in enumerate(sources):
        for x, r in enumerate(peers):
            remote(
                src.at[0, :, :, lanes(r - 1)], dst.at[x, here], kv_send.at[i], kv_recv.at[i],
                {"blk": flip(b, 1)},
            ).start()

    table_copy.wait()
    len_copy.wait()
    table = table_ref[0]
    seq_id = lax.broadcasted_iota(jnp.int32, table.shape, 0)
    place = lax.broadcasted_iota(jnp.int32, table.shape, 1)
    length = jnp.zeros(table.shape, jnp.int32)
    for q in range(seqs):
        length = jnp.where(seq_id == q, jnp.broadcast_to(len_ref[0:1, q : q + 1], table.shape), length)
    marked = jnp.where(place < length, table - b // 2 * 2 * slots, -1)
    row_seq = (lax.broadcasted_iota(jnp.int32, (period, LANES), 0) % tokens) // STEPS
    for s in range(2 * slots):
        owner = jnp.max(jnp.where(marked == s, seq_id, -1), axis=1, keepdims=True)
        owner = jnp.max(owner, axis=0, keepdims=True)
        owner = jnp.broadcast_to(owner, (period, LANES))
        bias_ref[s] = jnp.where(owner == row_seq, 0.0, empty_max)

    def take(d):
        z_copy(d).wait_recv()
        forward(flip(g, d))

    for d in order:
        if d in direct:
            pl.when(g > 0)(functools.partial(take, d))
        else:
            take(d)

    for i, (_, buf) in enumerate(sources):
        pltpu.make_async_copy(buf.at[:, here], buf.at[:, here], kv_sem.at[i]).wait()

    def unit(x):
        query = q_buf[x].astype(jnp.float32).reshape(rows, DH).astype(jnp.bfloat16)
        blank = jnp.zeros((rows, DH), jnp.bfloat16)
        both = jnp.concatenate(
            [jnp.concatenate([query, blank], axis=1), jnp.concatenate([blank, query], axis=1)], axis=0
        )
        step = 2 if slots % 2 == 0 else 1
        scores = []
        for s in range(0, slots, step):
            keys = jnp.concatenate(
                [k_buf[x, half * slots + s : half * slots + s + step].reshape(step * block, DH) for half in range(2)],
                axis=1,
            )
            out = lax.dot_general(
                both, keys, (((1,), (1,)), ((), ())), preferred_element_type=jnp.float32
            )
            scores += [out[:, i * block : (i + 1) * block] for i in range(step)]
        tops, totals = [], []
        for half in range(2):
            mine = []
            for s in range(slots):
                bias = jnp.concatenate([bias_ref[half * slots + s]] * (rows // period), axis=0)
                mine.append(scores[s][half * rows : (half + 1) * rows] * scale + bias)
            top = mine[0]
            for score in mine[1:]:
                top = jnp.maximum(top, score)
            top = jnp.broadcast_to(jnp.max(top, axis=1, keepdims=True), (rows, LANES))
            weights = jnp.concatenate([jnp.exp2(score - top).astype(jnp.bfloat16) for score in mine], axis=1)
            values = v_buf[x, half * slots : (half + 1) * slots].reshape(slots * block, DH)
            values = jnp.concatenate([values, jnp.ones(values.shape, jnp.bfloat16)], axis=1)
            totals.append(jnp.dot(weights, values, preferred_element_type=jnp.float32))
            tops.append(top)
        top = jnp.maximum(tops[0], tops[1])
        parts = [jnp.exp2(t - top) for t in tops]
        o = totals[0][:, :DH] * parts[0] + totals[1][:, :DH] * parts[1]
        total = totals[0][:, DH:] * parts[0] + totals[1][:, DH:] * parts[1]
        return o.astype(jnp.bfloat16), top, total

    def in_rows(top, total):
        lane = lax.broadcasted_iota(jnp.int32, (rows, LANES), 1)
        stats = jnp.where(lane == 0, top, total)
        stats = jnp.concatenate([stats, jnp.zeros((LANES - rows, LANES), jnp.float32)], axis=0)
        return jnp.transpose(stats)[:2]

    for i, (_, buf) in enumerate(sources):
        like(buf.at[:, here], kv_send.at[i], kv_recv.at[i]).wait_recv()

    for x in (0, 3, 1, 2):
        r = peers[x]
        if r:
            part = q_buf.at[x]
            like(part, p_send.at[0], p_recv.at[x]).wait_recv()
        o, top, total = unit(x)
        if r:
            o_send[x] = o
            remote(o_send.at[x], o_recv.at[x], o_ssem.at[0], o_rsem.at[0], {"blk": flip(b, r)}).start()
            s_send[x] = in_rows(top, total)
            remote(s_send.at[x], s_recv.at[x], s_ssem.at[0], s_rsem.at[0], {"blk": flip(b, r)}).start()
        else:
            o_recv[x] = o
            s_recv[x] = in_rows(top, total)

    others = pl.ds(0, units)
    like(s_recv.at[others], s_ssem.at[0], s_rsem.at[0]).wait_recv()
    tops = s_recv[:, 0, :]
    factor = jnp.exp2(tops - jnp.max(tops, axis=0, keepdims=True))
    share = factor / jnp.sum(factor * s_recv[:, 1, :], axis=0, keepdims=True)
    share = jnp.concatenate([share, jnp.zeros((LANES - units, LANES), jnp.float32)], axis=0)
    share = jnp.transpose(share)[:rows]
    like(o_recv.at[others], o_ssem.at[0], o_rsem.at[0]).wait_recv()
    merged = jnp.zeros((rows, DH), jnp.float32)
    for x in range(units):
        merged = merged + share[:, x : x + 1] * o_recv[x].astype(jnp.float32)
    o_rows[...] = merged
    for h in range(per_group):
        out_ref[:, h * DH : (h + 1) * DH] = o_rows[h * tokens : (h + 1) * tokens, :].astype(jnp.bfloat16)

    for d in order:
        if d in direct:
            pl.when(g != d)(z_copy(d).wait_send)
        else:
            z_copy(d).wait_send()
    for d in direct:
        @pl.when(g == d)
        def _():
            like(q_buf.at[pl.ds(0, len(cross)), 0], d_send.at[0], p_recv.at[0]).wait_send()

    @pl.when(g == 0)
    def _():
        part = q_buf.at[pl.ds(0, len(cross)), pl.ds(0, n_grp - len(direct))]
        like(part, p_send.at[0], p_recv.at[0]).wait_send()

    @pl.when(g > 0)
    def _():
        like(q_buf.at[pl.ds(0, len(cross))], p_send.at[0], p_recv.at[0]).wait_send()

    for i, (_, buf) in enumerate(sources):
        like(buf.at[:, here], kv_send.at[i], kv_recv.at[i]).wait_send()
    like(o_send.at[others], o_ssem.at[0], o_rsem.at[0]).wait_send()
    like(s_send.at[others], s_ssem.at[0], s_rsem.at[0]).wait_send()


def fused_body(n_blk, n_grp, queries, key_pool, value_pool, lengths, block_table):
    seqs = lengths.shape[1]
    tokens = seqs * STEPS
    heads = queries.shape[1] // DH
    per_group = HQ // KVH
    slots, block = key_pool.shape[1:3]
    rows = tokens * per_group
    blocks = tokens * heads // SUB
    units = n_blk // 2
    dma = pltpu.SemaphoreType.DMA
    vmem = pl.BlockSpec(memory_space=pltpu.VMEM)
    hbm = pl.BlockSpec(memory_space=pltpu.HBM)
    return pl.pallas_call(
        functools.partial(fused, n_blk, n_grp, seqs, tokens, heads, per_group),
        out_shape=pltpu.VMEM((tokens, per_group * DH), jnp.bfloat16),
        in_specs=[hbm] * 5,
        out_specs=vmem,
        scratch_shapes=[
            pltpu.VMEM(queries.shape, jnp.bfloat16),
            pltpu.VMEM(queries.shape, jnp.float32),
            pltpu.VMEM((n_grp, blocks, SUB, DH), jnp.bfloat16),
            pltpu.VMEM((n_grp, blocks, SUB, DH), jnp.bfloat16),
            pltpu.VMEM((units, n_grp, blocks, SUB, DH), jnp.bfloat16),
            pltpu.VMEM((units, 2 * slots, block, DH), jnp.bfloat16),
            pltpu.VMEM((units, 2 * slots, block, DH), jnp.bfloat16),
            pltpu.VMEM((units, rows, DH), jnp.bfloat16),
            pltpu.VMEM((units, rows, DH), jnp.bfloat16),
            pltpu.VMEM((units, 2, LANES), jnp.float32),
            pltpu.VMEM((units, 2, LANES), jnp.float32),
            pltpu.VMEM((rows, DH), jnp.float32),
            pltpu.VMEM(block_table.shape, jnp.int32),
            pltpu.VMEM(lengths.shape, jnp.int32),
            pltpu.VMEM((2 * slots, math.lcm(tokens, SUB), LANES), jnp.float32),
            dma((3,)), dma((2,)), dma((2,)), dma((2,)),
            dma((n_grp,)), dma((n_grp,)),
            dma((1,)), dma((units,)), dma((1,)),
            dma((1,)), dma((1,)), dma((1,)), dma((1,)),
        ],
        compiler_params=pltpu.CompilerParams(
            collective_id=0, has_side_effects=True, vmem_limit_bytes=62914560
        ),
    )(queries, key_pool, value_pool, lengths, block_table)


def choose(mesh):
    n_blk, n_grp = mesh.shape["blk"], mesh.shape["grp"]

    def run(queries, key_pool, value_pool, lengths, block_table):
        rows = lengths.shape[1] * HQ // KVH * STEPS
        fits = (
            n_blk == KVH
            and n_blk & (n_blk - 1) == 0
            and n_grp & (n_grp - 1) == 0
            and queries.shape[1] % DH == 0
            and (lengths.shape[1] * STEPS * queries.shape[1] // DH) % SUB == 0
            and rows % math.lcm(lengths.shape[1] * STEPS, SUB) == 0
            and rows % 16 == 0
            and rows <= LANES
            and key_pool.shape[2] == LANES
        )
        if not fits:
            return body(queries, key_pool, value_pool, lengths, block_table)
        return fused_body(n_blk, n_grp, queries, key_pool, value_pool, lengths, block_table)

    return run


def solution(mesh):
    placed = (
        P(None, ("blk", "grp")),
        P("grp", "blk", None, None),
        P("grp", "blk", None, None),
        P("grp", None),
        P("grp", None, None),
    )
    return jax.shard_map(
        choose(mesh), mesh=mesh, in_specs=placed, out_specs=P("grp", "blk"), check_vma=False
    )
```
